32 devices in a mesh: seq: 8 (over z, y), head: 4 (over x, core).
Axes of the slice: x: 2, y: 2, z: 4, core: 2. Of those that a mesh axis runs over, the one named last changes fastest.
Arguments:
- layer_in: bfloat16 [4096, 2048], P('seq', 'head'), may hold values from -6 to 6
- query_weight: bfloat16 [2048, 1024], P(None, 'head'), may hold values from -0.125 to 0.125
- key_weight: bfloat16 [2048, 1024], P(None, 'head'), may hold values from -0.125 to 0.125
- value_weight: bfloat16 [2048, 1024], P(None, 'head'), may hold values from -0.125 to 0.125
- gate_weight: bfloat16 [2048, 1024], P(None, 'head'), may hold values from -0.125 to 0.125
- beta_weight: bfloat16 [2048, 8], P(None, 'head'), may hold values from -0.125 to 0.125
- decay_weight: bfloat16 [2048, 8], P(None, 'head'), may hold values from -0.125 to 0.125
- conv_weight: float32 [4, 3, 1024], P(None, None, 'head'), may hold values from -3 to 3
- decay_log: float32 [8], P('head'), as said below
- beta_bias: float32 [8], P('head'), as said below
- decay_bias: float32 [8], P('head'), may hold values from -1 to 1
- norm_gain: float32 [128], replicated, may hold values from 0.1 to 1.9
- out_weight: bfloat16 [1024, 2048], P('head'), may hold values from -0.1875 to 0.1875
Outputs:
- layer_out: bfloat16 [4096, 2048], P('seq', 'head')
The draws below stay inside these ranges and needn't reach their ends.
Inputs may be any that keep to these rules, and one draw needn't show every extreme that they name: decay_log lies between log(0.1 / 4096) and log(0.05). beta_bias lies between log(0.5 * 128 / 4096) and 1.
All inputs are finite; a program needn't handle non-finite values.
Results may differ from the reference program's by a relative error of at most 0.0049.
Values may be sent and summed in bfloat16 or wider, within the bound.
A program may use at most 128 MiB of HBM per device.

```python
import jax
import jax.numpy as jnp
from jax import lax

D = 2048
HEADS = 8
HDIM = 128
CONV = 4
BLOCK = 128
TOKENS = 4096


def head_kinds(key):
    pair_count = HEADS // 2
    pick_one = jax.random.randint(jax.random.fold_in(key, 31), (pair_count,), 0, 2)
    rolled = jax.random.randint(jax.random.fold_in(key, 32), (pair_count,), 0, 100)
    limit = 25
    both_slow = rolled < limit
    first_slow = (pick_one == 0) | both_slow
    second_slow = (pick_one == 1) | both_slow
    return jnp.stack([first_slow, second_slow], axis=1).reshape(HEADS)


def draw_decay_log(key, part):
    slow_heads = head_kinds(key)
    spread = jax.random.uniform(jax.random.fold_in(key, 41), (HEADS,), jnp.float32)
    slow_rate = jnp.log((0.1 + 0.4 * spread) / TOKENS)
    fast_rate = jnp.log(0.02 + 0.03 * spread)
    return jnp.where(slow_heads, slow_rate, fast_rate).astype(jnp.float32)


def draw_beta_bias(key, part):
    slow_heads = head_kinds(key)
    spread = jax.random.uniform(jax.random.fold_in(key, 42), (HEADS,), jnp.float32)
    slow_bias = jnp.log((0.5 + 0.5 * spread) * HDIM / TOKENS)
    fast_bias = 2.0 * spread - 1.0
    return jnp.where(slow_heads, slow_bias, fast_bias).astype(jnp.float32)


def shard_levels(rng, shape, shards, smallest, high):
    loudness = 1.0
    for position, shards_of in shards:
        steps = jax.random.uniform(jax.random.fold_in(jax.random.fold_in(rng, 6), position), (shards_of,), jnp.float32, smallest / len(shards), high / len(shards))
        loudness = loudness * jnp.repeat(jnp.exp(steps), shape[position] // shards_of).reshape((-1,) + (1,) * (len(shape) - 1 - position))
    return loudness


def bell_draw(rng, extent, width, reach, pieces=(), kind=jnp.bfloat16):
    values = width * jax.random.normal(rng, extent, jnp.float32)
    if pieces:
        values = values * shard_levels(rng, extent, pieces, -0.22, 0.18)
    return jnp.clip(values, -reach, reach).astype(kind)


def setup_inputs(seed: int = 0) -> dict:
    seeds = jax.random.split(jax.random.key(seed), 14)
    layer_in = bell_draw(seeds[0], (TOKENS, D), 1.0, 6.0, ((0, 8), (1, 4)))
    query_weight = bell_draw(seeds[1], (D, HEADS * HDIM), D ** -0.5, 0.125, ((1, 4),))
    key_weight = bell_draw(seeds[2], (D, HEADS * HDIM), D ** -0.5, 0.125, ((1, 4),))
    value_weight = bell_draw(seeds[3], (D, HEADS * HDIM), D ** -0.5, 0.125, ((1, 4),))
    gate_weight = bell_draw(seeds[4], (D, HEADS * HDIM), D ** -0.5, 0.125, ((1, 4),))
    beta_weight = bell_draw(seeds[5], (D, HEADS), D ** -0.5, 0.125, ((1, 4),))
    decay_weight = bell_draw(seeds[6], (D, HEADS), D ** -0.5, 0.125, ((1, 4),))
    conv_weight = bell_draw(seeds[7], (CONV, 3, HEADS * HDIM), 0.5, 3.0, ((2, 4),), jnp.float32)
    decay_log = draw_decay_log(jax.random.fold_in(seeds[13], 71), 0)
    beta_bias = draw_beta_bias(jax.random.fold_in(seeds[13], 71), 0)
    decay_bias = jnp.clip(jax.random.uniform(seeds[10], (HEADS,), jnp.float32, -1.0, 1.0) * shard_levels(seeds[10], (HEADS,), ((0, 4),), -0.4, 0.0), -1.0, 1.0)
    norm_gain = jnp.clip(1.0 + 0.18 * jax.random.normal(seeds[11], (HDIM,), jnp.float32), 0.1, 1.9)
    out_weight = bell_draw(seeds[12], (HEADS * HDIM, D), (HEADS * HDIM) ** -0.5, 0.1875, ((0, 4),))
    return {"layer_in": layer_in, "query_weight": query_weight, "key_weight": key_weight, "value_weight": value_weight, "gate_weight": gate_weight, "beta_weight": beta_weight, "decay_weight": decay_weight, "conv_weight": conv_weight, "decay_log": decay_log, "beta_bias": beta_bias, "decay_bias": decay_bias, "norm_gain": norm_gain, "out_weight": out_weight}


exact_mode = lax.Precision.HIGHEST
norm_floor = 0.0001

def causal_conv(values, kernel):
    taps = kernel.shape[0]
    summed = kernel[0] * values
    for offset in range(1, taps):
        shifted = jnp.concatenate([jnp.zeros((offset, values.shape[1]), jnp.float32), values[:-offset]], axis=0)
        summed = summed + kernel[offset] * shifted
    return jax.nn.silu(summed)

def unit_rows(values):
    return values * lax.rsqrt(lax.optimization_barrier(jnp.sum(values * values, axis=-1, keepdims=True)) + 1.0)

def block_terms(queries, key_rows, values, beta_gate, log_decay):
    length = log_decay.shape[-1]
    running = jnp.cumsum(log_decay, axis=-1)
    row_index = lax.broadcasted_iota(jnp.int32, (length, length), 0)
    col_index = lax.broadcasted_iota(jnp.int32, (length, length), 1)
    within = row_index >= col_index
    before = row_index > col_index
    spread = running[..., :, None] - running[..., None, :]
    decay_matrix = jnp.where(within, jnp.exp(jnp.minimum(spread, 0.0)), 0.0)
    key_gram = jnp.einsum('...rd,...sd->...rs', key_rows, key_rows, precision=exact_mode)
    lower_part = jnp.where(before, beta_gate[..., :, None] * decay_matrix * key_gram, 0.0)
    system = lower_part + jnp.eye(length, dtype=jnp.float32)
    growth = jnp.exp(running)
    right_side = jnp.concatenate([beta_gate[..., None] * values, (beta_gate * growth)[..., None] * key_rows], axis=-1)
    solved = lax.linalg.triangular_solve(system, right_side, left_side=True, lower=True, unit_diagonal=True)
    value_dim = values.shape[-1]
    fixed_rows = solved[..., :value_dim]
    erased = solved[..., value_dim:]
    query_key = jnp.einsum('...rd,...sd->...rs', queries, key_rows, precision=exact_mode)
    mixing = jnp.where(within, decay_matrix * query_key, 0.0)
    local_out = jnp.einsum('...rs,...se->...re', mixing, fixed_rows, precision=exact_mode)
    reader = growth[..., None] * queries - jnp.einsum('...rs,...sd->...rd', mixing, erased, precision=exact_mode)
    tail_decay = jnp.exp(running[..., -1:] - running)
    weighted = tail_decay[..., None] * key_rows
    key_dim = key_rows.shape[-1]
    transit = jnp.exp(running[..., -1])[..., None, None] * jnp.eye(key_dim, dtype=jnp.float32) - jnp.einsum('...bd,...be->...de', weighted, erased, precision=exact_mode)
    carried = jnp.einsum('...bd,...be->...de', weighted, fixed_rows, precision=exact_mode)
    return (local_out, reader, transit, carried)

def reference(layer_in, query_weight, key_weight, value_weight, gate_weight, beta_weight, decay_weight, conv_weight, decay_log, beta_bias, decay_bias, norm_gain, out_weight):
    tokens = layer_in.shape[0]

    def project(weight):
        return jnp.dot(layer_in.astype(jnp.float32), weight.astype(jnp.float32), preferred_element_type=jnp.float32)
    mixed_query = causal_conv(project(query_weight), conv_weight[:, 0])
    mixed_key = causal_conv(project(key_weight), conv_weight[:, 1])
    mixed_value = causal_conv(project(value_weight), conv_weight[:, 2])
    queries = unit_rows(mixed_query.reshape(tokens, HEADS, HDIM))
    key_rows = unit_rows(mixed_key.reshape(tokens, HEADS, HDIM))
    values = mixed_value.reshape(tokens, HEADS, HDIM)
    beta_gate = jax.nn.sigmoid(project(beta_weight) + beta_bias)
    log_decay = -jnp.exp(decay_log) * jax.nn.softplus(project(decay_weight) + decay_bias)
    blocks = tokens // BLOCK

    def arrange(array):
        return array.reshape(blocks, BLOCK, HEADS, HDIM).transpose(0, 2, 1, 3)

    def arrange_gate(array):
        return array.reshape(blocks, BLOCK, HEADS).transpose(0, 2, 1)

    def advance(carry_state, inputs):
        local_out, reader, transit, carried = block_terms(*inputs)
        output = local_out + jnp.einsum('hrd,hde->hre', reader, carry_state, precision=exact_mode)
        carry_state = jnp.einsum('hde,hef->hdf', transit, carry_state, precision=exact_mode) + carried
        return (carry_state, output)
    zero_state = jnp.zeros((HEADS, HDIM, HDIM), jnp.float32)
    last_state, outputs = lax.scan(advance, zero_state, (arrange(queries), arrange(key_rows), arrange(values), arrange_gate(beta_gate), arrange_gate(log_decay)))
    head_out = outputs.transpose(0, 2, 1, 3).reshape(tokens, HEADS, HDIM)
    gate_rows = project(gate_weight).reshape(tokens, HEADS, HDIM)
    scaled = head_out * lax.rsqrt(lax.optimization_barrier(jnp.mean(head_out * head_out, axis=-1, keepdims=True)) + norm_floor)
    hidden = (scaled * norm_gain * jax.nn.silu(gate_rows)).reshape(tokens, HEADS * HDIM).astype(jnp.bfloat16)
    return jnp.dot(hidden.astype(jnp.float32), out_weight.astype(jnp.float32), preferred_element_type=jnp.float32).astype(jnp.bfloat16)
```

```python
import functools

import jax
import jax.numpy as jnp
from jax import lax
from jax.experimental import pallas as pl
from jax.experimental.pallas import tpu as pltpu
from jax.sharding import PartitionSpec as P

BLOCK = 128
PRIOR = 16
LANES = 128
GROUPS = 2
PER_GROUP = 2
MESH = pl.DeviceIdType.MESH
F32 = jnp.float32
BF16 = jnp.bfloat16
norm_floor = 0.0001


def bits_below(limit):
    found = []
    bit = limit // 2
    while bit:
        found.append(bit)
        bit //= 2
    return found


def low_bit(value):
    return value & -value


def meet(peers):
    barrier = pltpu.get_barrier_semaphore()
    expected = 0
    for present, device in peers:
        if present is True:
            pl.semaphore_signal(barrier, inc=1, device_id=device, device_id_type=MESH)
            expected = expected + 1
        else:

            @pl.when(present)
            def _():
                pl.semaphore_signal(barrier, inc=1, device_id=device, device_id_type=MESH)

            expected = expected + present.astype(jnp.int32)
    pl.semaphore_wait(barrier, expected)


def remote(source, target, send_sem, recv_sem, device):
    return pltpu.make_async_remote_copy(
        src_ref=source,
        dst_ref=target,
        send_sem=send_sem,
        recv_sem=recv_sem,
        device_id=device,
        device_id_type=MESH,
    )


def dot(left, right, contract=((1,), (0,))):
    return lax.dot_general(
        left.astype(BF16), right.astype(BF16), (contract, ((), ())), preferred_element_type=F32
    )


def split(value):
    high = value.astype(BF16)
    return high, (value - high.astype(F32)).astype(BF16)


def dot3(left, right, contract=((1,), (0,))):
    lh, ll = left if isinstance(left, tuple) else split(left)
    rh, rl = right if isinstance(right, tuple) else split(right)
    axis = contract[1][0]
    both = dot(jnp.concatenate([lh, lh], axis=1), jnp.concatenate([rh, rl], axis=axis), contract)
    return both + dot(ll, rh, contract)


def layer_kernel(
    seqs, n, heads,
    x_ref, wq, wk, wv, wg, beta_ref, step_ref, taps, rates, beta_bias, decay_bias, gain, w_ref,
    out_ref,
    w_all, w_flat, x_own, buf, prior, raw, local, reader, maps, slab,
    w_buf, pair_buf, go_buf, in_buf, hid,
    load_sem, x_sem, x_send, x_recv, p_send, p_recv, own_sem, w_send, w_recv,
    pair_sem, chain_send, chain_recv, h_send, h_recv,
):
    seq = lax.axis_index("seq")
    me = lax.axis_index("head")
    tokens, feats = x_ref.shape
    width = wq.shape[1]
    dim = LANES
    blocks = tokens // BLOCK
    columns = out_ref.shape[1]
    sends_each = GROUPS * PER_GROUP
    rows = tokens // sends_each
    group_rows = tokens // GROUPS
    group_blocks = blocks // GROUPS
    bits = bits_below(n)

    loads = [pltpu.make_async_copy(x_ref, x_own, x_sem)]
    for i, w in enumerate((wq, wk, wv, wg)):
        loads.append(
            pltpu.make_async_copy(w, w_all.at[:, pl.ds(i * width, width)], load_sem.at[i])
        )
    for load in loads:
        load.start()
    has_next = seq < seqs - 1
    has_before = seq > 0
    far_next = seq < seqs - 2
    far_before = seq >= 2
    odd = seq % 2
    is_odd = odd == 1
    mate = seq + 1 - 2 * odd
    peers = [(True, (seq, me ^ m)) for m in range(1, n)]
    peers += [(has_next, (seq + 1, me ^ m)) for m in range(n)]
    peers += [(has_before, (seq - 1, me ^ m)) for m in range(n)]
    peers += [(far_next, (seq + 2, me)), (far_before, (seq - 2, me))]
    meet(peers)

    def hop(m, bit, c):
        piece = pl.ds(c * rows, rows)
        source = x_ref.at[piece] if m == 0 else buf.at[m, piece]
        got = m | bit
        return remote(
            source, buf.at[got, piece], x_send.at[got, c], x_recv.at[got, c], (seq, me ^ bit)
        )

    hops = {}
    for bit in bits:
        for c in range(sends_each):
            hops[bit, c] = hop(0, bit, c)
            hops[bit, c].start()
    tails = [
        remote(
            x_ref.at[pl.ds(tokens - PRIOR, PRIOR)],
            prior.at[m],
            p_send.at[m],
            p_recv.at[m],
            (seq + 1, me ^ m),
        )
        for m in range(n)
    ]

    @pl.when(has_next)
    def _():
        for tail in tails:
            tail.start()

    w_flat[...] = jnp.zeros(w_flat.shape, F32)
    w_flat[pl.ds(0, heads), :] = beta_ref[...].astype(F32)
    w_flat[pl.ds(heads, heads), :] = step_ref[...].astype(F32)
    for i in range(w_flat.shape[1] // LANES):
        piece = pl.ds(i * LANES, LANES)
        w_all[piece, pl.ds(4 * width, LANES)] = w_flat[:, piece].T.astype(BF16)
    for load in loads:
        load.wait()

    def weights_of(m):
        start = pl.multiple_of((me ^ m) * feats, LANES)
        return w_all[pl.ds(start, feats), :]

    def arrive(m, c):
        hops[m, c].wait_recv()
        for bit in bits:
            if bit < low_bit(m):
                hops[m | bit, c] = hop(m, bit, c)
                hops[m | bit, c].start()

    def add(m, g):
        piece = pl.ds(g * group_rows, group_rows)
        here = pl.ds(PRIOR + g * group_rows, group_rows)
        values = x_own[piece, :] if m == 0 else buf[m, piece, :]
        term = jnp.dot(values, weights_of(m), preferred_element_type=F32)
        if m == 0:
            raw[here, :] = term
        else:
            raw[here, :] = raw[here, :] + term

    for g in range(GROUPS):
        add(0, g)
    for g in range(GROUPS):
        for c in range(g * PER_GROUP, (g + 1) * PER_GROUP):
            arrive(1, c)
        add(1, g)

    @pl.when(has_before)
    def _():
        total = jnp.zeros((PRIOR, raw.shape[1]), F32)
        for m in range(n):
            tails[m].wait_recv()
            total = total + jnp.dot(prior[m], weights_of(m), preferred_element_type=F32)
        raw[pl.ds(0, PRIOR), :] = total

    @pl.when(jnp.logical_not(has_before))
    def _():
        raw[pl.ds(0, PRIOR), :] = jnp.zeros((PRIOR, raw.shape[1]), F32)

    row = lax.broadcasted_iota(jnp.int32, (BLOCK, BLOCK), 0)
    col = lax.broadcasted_iota(jnp.int32, (BLOCK, BLOCK), 1)
    within = row >= col
    before = row > col
    eye = (row == col).astype(F32)
    lower = within.astype(F32)
    lane = lax.broadcasted_iota(jnp.int32, (1, LANES), 1)
    offset = jnp.zeros((1, LANES), F32)
    rate = jnp.zeros((1, LANES), F32)
    for h in range(heads):
        offset = jnp.where(lane == h, beta_bias[h], offset)
        offset = jnp.where(lane == heads + h, decay_bias[h], offset)
        rate = jnp.where(lane == heads + h, rates[h], rate)
    rate = -jnp.exp(rate)

    def mixed(kind, h, b):
        base = kind * width + h * dim
        start = PRIOR + b * BLOCK
        total = None
        for s in range(taps.shape[1]):
            tap = taps[kind, pl.ds(s, 1), pl.ds(h * dim, dim)]
            term = tap * raw[pl.ds(start - s, BLOCK), pl.ds(base, dim)]
            total = term if total is None else total + term
        return total * jax.nn.sigmoid(total)

    def unit(values):
        return values * lax.rsqrt(jnp.sum(values * values, axis=-1, keepdims=True) + 1.0)

    def block_terms(g, midway):
        pairs = [(b, h) for b in range(g * group_blocks, (g + 1) * group_blocks)
                 for h in range(heads)]
        betas, runs, acrosses = {}, {}, {}
        for b in range(g * group_blocks, (g + 1) * group_blocks):
            small = raw[pl.ds(PRIOR + b * BLOCK, BLOCK), pl.ds(4 * width, LANES)] + offset
            betas[b] = jax.nn.sigmoid(small)
            steps = rate * (jnp.maximum(small, 0.0) + jnp.log1p(jnp.exp(-jnp.abs(small))))
            runs[b] = jnp.dot(
                lower, steps, precision=lax.Precision.HIGHEST, preferred_element_type=F32
            )
            acrosses[b] = runs[b].T
        lows, mixes, sides, weighteds, reads, ends = [], [], [], [], [], []
        for b, h in pairs:
            q = unit(mixed(0, h, b))
            k = unit(mixed(1, h, b))
            v = mixed(2, h, b)
            beta = betas[b][:, h : h + 1]
            down = runs[b][:, heads + h : heads + h + 1]
            along = acrosses[b][heads + h : heads + h + 1, :]
            last = down[BLOCK - 1 : BLOCK, :]
            decay = jnp.where(within, jnp.exp(jnp.minimum(down - along, 0.0)), 0.0)
            grams = dot3(jnp.concatenate([q, k], axis=0), k, ((1,), (1,)))
            mixes.append(decay * grams[:BLOCK])
            lows.append(jnp.where(before, beta * decay * grams[BLOCK:], 0.0))
            growth = jnp.exp(down)
            sides.append(jnp.concatenate([beta * v, (beta * growth) * k], axis=1))
            weighteds.append((jnp.exp(last - down) * k).T)
            reads.append(growth * q)
            ends.append(jnp.exp(last))
        inverses = [eye - jnp.where((row // 2 == col // 2), low, 0.0) for low in lows]
        span = 2
        while span < BLOCK:
            linked = (row // (2 * span) == col // (2 * span)) & (row // span > col // span)
            shares = [split(inv) for inv in inverses]
            middles = [
                dot3(jnp.where(linked, low, 0.0), share) for low, share in zip(lows, shares)
            ]
            inverses = [
                inv - dot3(share, middle)
                for inv, share, middle in zip(inverses, shares, middles)
            ]
            span *= 2
        midway()
        solved = [split(dot3(inv, side)) for inv, side in zip(inverses, sides)]
        found = {}
        for i, (b, h) in enumerate(pairs):
            got = dot3(weighteds[i], solved[i])
            transit = ends[i] * eye - got[:, dim:]
            reader[h, b, pl.ds(BLOCK, dim), :] = transit.astype(BF16)
            maps[h, b] = got[:, :dim]
            found[b, h] = (transit, got[:, :dim])

        def outputs():
            for i, (b, h) in enumerate(pairs):
                got = dot3(mixes[i], solved[i])
                local[h, pl.ds(b * BLOCK, BLOCK), :] = got[:, :dim]
                reader[h, b, pl.ds(0, BLOCK), :] = (reads[i] - got[:, dim:]).astype(BF16)

        return found, outputs

    far = sorted(range(2, n), key=lambda m: (-low_bit(m), m))
    joined = [None] * heads
    for g in range(GROUPS):
        mine = range(g * PER_GROUP, (g + 1) * PER_GROUP)
        for m in far:
            for c in mine:
                if (m, "in", c) not in hops:
                    arrive(m, c)
            add(m, g)

        def midway():
            if g + 1 < GROUPS:
                for m in far:
                    if low_bit(m) > 1:
                        c = (g + 1) * PER_GROUP
                        arrive(m, c)
                        hops[m, "in", c] = None

        found, outputs = block_terms(g, midway)
        for h in range(heads):
            for b in range(g * group_blocks, (g + 1) * group_blocks):
                transit, carried = found[b, h]
                if joined[h] is None:
                    joined[h] = jnp.concatenate([transit, carried], axis=1)
                else:
                    moved = dot3(transit, joined[h])
                    joined[h] = jnp.concatenate(
                        [moved[:, :dim], moved[:, dim:] + carried], axis=1
                    )
        if g + 1 < GROUPS:
            outputs()
        else:
            for h in range(heads):
                slab[h] = joined[h].astype(slab.dtype)

    swaps = [
        remote(slab.at[h], pair_buf.at[h], pair_sem.at[0, h], pair_sem.at[1, h], (mate, me))
        for h in range(heads)
    ]
    for swap in swaps:
        swap.start()

    def columns_of(m):
        return pl.ds(pl.multiple_of((me ^ m) * columns, LANES), columns)

    own = pltpu.make_async_copy(w_ref.at[:, columns_of(0)], w_buf.at[0], own_sem)
    own.start()
    moves = []
    for m in range(1, n):
        move = remote(
            w_ref.at[:, columns_of(m)], w_buf.at[m], w_send.at[m], w_recv.at[m], (seq, me ^ m)
        )
        move.start()
        moves.append(move)
    outputs()

    firsts, comps = [], []
    for h in range(heads):
        swaps[h].wait()
        here = slab[h].astype(F32)
        there = pair_buf[h].astype(F32)
        first = jnp.where(is_odd, there, here)
        second = jnp.where(is_odd, here, there)
        moved = dot(second[:, :dim], first)
        comps.append((moved[:, :dim], moved[:, dim:] + second[:, dim:]))
        firsts.append(first)
    sends = [
        remote(go_buf.at[h], in_buf.at[h], chain_send.at[h], chain_recv.at[h], (seq + 2, me))
        for h in range(heads)
    ]

    @pl.when(jnp.logical_not(far_before))
    def _():
        in_buf[...] = jnp.zeros(in_buf.shape, in_buf.dtype)

    for h in range(heads):

        @pl.when(far_before)
        def _():
            sends[h].wait_recv()

        @pl.when(far_next)
        def _():
            go_buf[h] = (dot(comps[h][0], in_buf[h]) + comps[h][1]).astype(go_buf.dtype)
            sends[h].start()

    states = []
    for h in range(heads):
        arrived = in_buf[h].astype(F32)
        later = dot(firsts[h][:, :dim], arrived) + firsts[h][:, dim:]
        states.append(jnp.where(is_odd, later, arrived))

    lifts = {}

    def lift(m, bit, b):
        got = m | bit
        return remote(
            hid.at[m, b], hid.at[got, b], h_send.at[got, b], h_recv.at[got, b], (seq, me ^ bit)
        )

    def forward(m, b):
        limit = n if m == 0 else low_bit(m)
        for bit in bits:
            if bit < limit:
                lifts[m | bit, b] = lift(m, bit, b)
                lifts[m | bit, b].start()

    for b in range(blocks):
        for h in range(heads):
            got = dot(reader[h, b], states[h])
            states[h] = got[BLOCK:] + maps[h, b]
            head_out = got[:BLOCK] + local[h, pl.ds(b * BLOCK, BLOCK), :]
            gate = raw[pl.ds(PRIOR + b * BLOCK, BLOCK), pl.ds(3 * width + h * dim, dim)]
            scaled = head_out * lax.rsqrt(
                jnp.mean(head_out * head_out, axis=-1, keepdims=True) + norm_floor
            )
            hid[0, b, :, pl.ds(h * dim, dim)] = (
                scaled * gain[...] * (gate * jax.nn.sigmoid(gate))
            ).astype(BF16)
        forward(0, b)

    own.wait()
    for move in moves:
        move.wait()
    order = sorted(range(1, n), key=lambda m: (m != 1, -low_bit(m), m))
    for b in range(blocks):
        total = jnp.dot(hid[0, b], w_buf[0], preferred_element_type=F32)
        for m in order:
            lifts[m, b].wait_recv()
            forward(m, b)
            total = total + jnp.dot(hid[m, b], w_buf[m], preferred_element_type=F32)
        out_ref[pl.ds(b * BLOCK, BLOCK), :] = total.astype(BF16)

    for key, copy in hops.items():
        if copy is not None:
            copy.wait_send()
    for copy in lifts.values():
        copy.wait_send()

    @pl.when(has_next)
    def _():
        for tail in tails:
            tail.wait_send()

    @pl.when(far_next)
    def _():
        for send in sends:
            send.wait_send()


def on_device(
    seqs, n,
    layer_in, query_weight, key_weight, value_weight, gate_weight, beta_weight, decay_weight,
    conv_weight, decay_log, beta_bias, decay_bias, norm_gain, out_weight,
):
    tokens, feats = layer_in.shape
    model, width = query_weight.shape
    heads = beta_weight.shape[1]
    dim = width // heads
    blocks = tokens // BLOCK
    total_width = 4 * width + LANES
    columns = out_weight.shape[1] // n
    vmem = pl.BlockSpec(memory_space=pltpu.VMEM)
    smem = pl.BlockSpec(memory_space=pltpu.SMEM)
    anywhere = pl.BlockSpec(memory_space=pl.ANY)
    dma = pltpu.SemaphoreType.DMA
    sends_each = GROUPS * PER_GROUP
    wire = BF16 if seqs <= 8 else F32
    return pl.pallas_call(
        functools.partial(layer_kernel, seqs, n, heads),
        out_shape=jax.ShapeDtypeStruct((tokens, columns), BF16),
        in_specs=[anywhere] * 5 + [vmem] * 3 + [smem] * 3 + [vmem, anywhere],
        out_specs=vmem,
        scratch_shapes=[
            pltpu.VMEM((model, total_width), BF16),
            pltpu.VMEM((LANES, model), F32),
            pltpu.VMEM((tokens, feats), BF16),
            pltpu.VMEM((n, tokens, feats), BF16),
            pltpu.VMEM((n, PRIOR, feats), BF16),
            pltpu.VMEM((PRIOR + tokens, total_width), F32),
            pltpu.VMEM((heads, tokens, dim), F32),
            pltpu.VMEM((heads, blocks, BLOCK + dim, dim), BF16),
            pltpu.VMEM((heads, blocks, dim, dim), F32),
            pltpu.VMEM((heads, dim, 2 * dim), wire),
            pltpu.VMEM((n, width, columns), BF16),
            pltpu.VMEM((heads, dim, 2 * dim), wire),
            pltpu.VMEM((heads, dim, dim), wire),
            pltpu.VMEM((heads, dim, dim), wire),
            pltpu.VMEM((n, blocks, BLOCK, width), BF16),
            dma((4,)),
            dma(()),
            dma((n, sends_each)),
            dma((n, sends_each)),
            dma((n,)),
            dma((n,)),
            dma(()),
            dma((n,)),
            dma((n,)),
            dma((2, heads)),
            dma((heads,)),
            dma((heads,)),
            dma((n, blocks)),
            dma((n, blocks)),
        ],
        compiler_params=pltpu.CompilerParams(
            collective_id=0, has_side_effects=True, vmem_limit_bytes=60 * 1024 * 1024
        ),
    )(
        layer_in, query_weight, key_weight, value_weight, gate_weight,
        beta_weight.T, decay_weight.T, conv_weight.transpose(1, 0, 2),
        decay_log, beta_bias, decay_bias, norm_gain[None], out_weight,
    )


def solution(mesh):
    return jax.shard_map(
        functools.partial(on_device, mesh.shape["seq"], mesh.shape["head"]),
        mesh=mesh,
        in_specs=(
            P("seq", "head"),
            P(None, "head"),
            P(None, "head"),
            P(None, "head"),
            P(None, "head"),
            P(None, "head"),
            P(None, "head"),
            P(None, None, "head"),
            P("head"),
            P("head"),
            P("head"),
            P(),
            P("head", None),
        ),
        out_specs=P("seq", "head"),
        check_vma=False,
    )
```

```python
import functools

import jax
import jax.numpy as jnp
from jax import lax
from jax.experimental import pallas as pl
from jax.experimental.pallas import tpu as pltpu
from jax.sharding import PartitionSpec as P

BLOCK = 128
PRIOR = 16
LANES = 128
GROUPS = 2
PER_GROUP = 2
MESH = pl.DeviceIdType.MESH
F32 = jnp.float32
BF16 = jnp.bfloat16
norm_floor = 0.0001


def bits_below(limit):
    found = []
    bit = limit // 2
    while bit:
        found.append(bit)
        bit //= 2
    return found


def low_bit(value):
    return value & -value


def meet(peers):
    barrier = pltpu.get_barrier_semaphore()
    expected = 0
    for present, device in peers:
        if present is True:
            pl.semaphore_signal(barrier, inc=1, device_id=device, device_id_type=MESH)
            expected = expected + 1
        else:

            @pl.when(present)
            def _():
                pl.semaphore_signal(barrier, inc=1, device_id=device, device_id_type=MESH)

            expected = expected + present.astype(jnp.int32)
    pl.semaphore_wait(barrier, expected)


def remote(source, target, send_sem, recv_sem, device):
    return pltpu.make_async_remote_copy(
        src_ref=source,
        dst_ref=target,
        send_sem=send_sem,
        recv_sem=recv_sem,
        device_id=device,
        device_id_type=MESH,
    )


def dot(left, right, contract=((1,), (0,))):
    return lax.dot_general(
        left.astype(BF16), right.astype(BF16), (contract, ((), ())), preferred_element_type=F32
    )


def split(value):
    high = value.astype(BF16)
    return high, (value - high.astype(F32)).astype(BF16)


def dot3(left, right, contract=((1,), (0,))):
    lh, ll = left if isinstance(left, tuple) else split(left)
    rh, rl = right if isinstance(right, tuple) else split(right)
    axis = contract[1][0]
    both = dot(jnp.concatenate([lh, lh], axis=1), jnp.concatenate([rh, rl], axis=axis), contract)
    return both + dot(ll, rh, contract)


def layer_kernel(
    seqs, n, heads,
    x_ref, wq, wk, wv, wg, beta_in, step_in, taps_in, rates_in, bias_in, shift_in, gain_in, w_ref,
    out_ref,
    w_all, w_flat, x_own, buf, prior, raw, local, reader, maps, slab,
    w_buf, pair_buf, go_buf, in_buf, hid,
    beta_ref, step_ref, taps, gain, rates, beta_bias, decay_bias,
    load_sem, small_sem, x_sem, x_send, x_recv, p_send, p_recv, own_sem, w_send, w_recv,
    pair_sem, chain_send, chain_recv, h_send, h_recv,
):
    seq = lax.axis_index("seq")
    me = lax.axis_index("head")
    tokens, feats = x_ref.shape
    width = wq.shape[1]
    dim = LANES
    blocks = tokens // BLOCK
    columns = out_ref.shape[1]
    sends_each = GROUPS * PER_GROUP
    rows = tokens // sends_each
    group_rows = tokens // GROUPS
    group_blocks = blocks // GROUPS
    bits = bits_below(n)

    loads = [pltpu.make_async_copy(x_ref, x_own, x_sem)]
    for i, w in enumerate((wq, wk, wv, wg)):
        loads.append(
            pltpu.make_async_copy(w, w_all.at[:, pl.ds(i * width, width)], load_sem.at[i])
        )
    smalls = [
        pltpu.make_async_copy(source, target, small_sem.at[i])
        for i, (source, target) in enumerate((
            (beta_in, beta_ref), (step_in, step_ref), (taps_in, taps), (gain_in, gain),
            (rates_in, rates), (bias_in, beta_bias), (shift_in, decay_bias),
        ))
    ]
    for load in loads + smalls:
        load.start()
    has_next = seq < seqs - 1
    has_before = seq > 0
    far_next = seq < seqs - 2
    far_before = seq >= 2
    odd = seq % 2
    is_odd = odd == 1
    mate = seq + 1 - 2 * odd
    peers = [(True, (seq, me ^ m)) for m in range(1, n)]
    peers += [(has_next, (seq + 1, me ^ m)) for m in range(n)]
    peers += [(has_before, (seq - 1, me ^ m)) for m in range(n)]
    peers += [(far_next, (seq + 2, me)), (far_before, (seq - 2, me))]
    meet(peers)

    def hop(m, bit, c):
        piece = pl.ds(c * rows, rows)
        source = x_ref.at[piece] if m == 0 else buf.at[m, piece]
        got = m | bit
        return remote(
            source, buf.at[got, piece], x_send.at[got, c], x_recv.at[got, c], (seq, me ^ bit)
        )

    tails = [
        remote(
            x_ref.at[pl.ds(tokens - PRIOR, PRIOR)],
            prior.at[m],
            p_send.at[m],
            p_recv.at[m],
            (seq + 1, me ^ m),
        )
        for m in range(n)
    ]

    @pl.when(has_next)
    def _():
        for tail in tails:
            tail.start()

    hops = {}
    for bit in bits:
        for c in range(sends_each):
            hops[bit, c] = hop(0, bit, c)
            hops[bit, c].start()
    for load in smalls:
        load.wait()
    w_flat[...] = jnp.zeros(w_flat.shape, F32)
    w_flat[pl.ds(0, heads), :] = beta_ref[...].astype(F32)
    w_flat[pl.ds(heads, heads), :] = step_ref[...].astype(F32)
    for i in range(w_flat.shape[1] // LANES):
        piece = pl.ds(i * LANES, LANES)
        w_all[piece, pl.ds(4 * width, LANES)] = w_flat[:, piece].T.astype(BF16)
    for load in loads:
        load.wait()

    def weights_of(m):
        start = pl.multiple_of((me ^ m) * feats, LANES)
        return w_all[pl.ds(start, feats), :]

    def arrive(m, c):
        hops[m, c].wait_recv()
        for bit in bits:
            if bit < low_bit(m):
                hops[m | bit, c] = hop(m, bit, c)
                hops[m | bit, c].start()

    def add(m, g):
        piece = pl.ds(g * group_rows, group_rows)
        here = pl.ds(PRIOR + g * group_rows, group_rows)
        values = x_own[piece, :] if m == 0 else buf[m, piece, :]
        term = jnp.dot(values, weights_of(m), preferred_element_type=F32)
        if m == 0:
            raw[here, :] = term
        else:
            raw[here, :] = raw[here, :] + term

    for g in range(GROUPS):
        add(0, g)
    for g in range(GROUPS):
        for c in range(g * PER_GROUP, (g + 1) * PER_GROUP):
            arrive(1, c)
        add(1, g)

    def add_prior():
        @pl.when(has_before)
        def _():
            total = jnp.zeros((PRIOR, raw.shape[1]), F32)
            for m in range(n):
                tails[m].wait_recv()
                total = total + jnp.dot(prior[m], weights_of(m), preferred_element_type=F32)
            raw[pl.ds(0, PRIOR), :] = total

        @pl.when(jnp.logical_not(has_before))
        def _():
            raw[pl.ds(0, PRIOR), :] = jnp.zeros((PRIOR, raw.shape[1]), F32)

    row = lax.broadcasted_iota(jnp.int32, (BLOCK, BLOCK), 0)
    col = lax.broadcasted_iota(jnp.int32, (BLOCK, BLOCK), 1)
    within = row >= col
    before = row > col
    eye = (row == col).astype(F32)
    lower = within.astype(F32)
    lane = lax.broadcasted_iota(jnp.int32, (1, LANES), 1)
    offset = jnp.zeros((1, LANES), F32)
    rate = jnp.zeros((1, LANES), F32)
    for h in range(heads):
        offset = jnp.where(lane == h, beta_bias[h], offset)
        offset = jnp.where(lane == heads + h, decay_bias[h], offset)
        rate = jnp.where(lane == heads + h, rates[h], rate)
    rate = -jnp.exp(rate)

    def mixed(kind, h, b):
        base = kind * width + h * dim
        start = PRIOR + b * BLOCK
        total = None
        for s in range(taps.shape[1]):
            tap = taps[kind, pl.ds(s, 1), pl.ds(h * dim, dim)]
            term = tap * raw[pl.ds(start - s, BLOCK), pl.ds(base, dim)]
            total = term if total is None else total + term
        return total * jax.nn.sigmoid(total)

    def unit(values):
        return values * lax.rsqrt(jnp.sum(values * values, axis=-1, keepdims=True) + 1.0)

    def block_terms(g, midway):
        pairs = [(b, h) for b in range(g * group_blocks, (g + 1) * group_blocks)
                 for h in range(heads)]
        betas, runs, acrosses = {}, {}, {}
        for b in range(g * group_blocks, (g + 1) * group_blocks):
            small = raw[pl.ds(PRIOR + b * BLOCK, BLOCK), pl.ds(4 * width, LANES)] + offset
            betas[b] = jax.nn.sigmoid(small)
            steps = rate * (jnp.maximum(small, 0.0) + jnp.log1p(jnp.exp(-jnp.abs(small))))
            runs[b] = jnp.dot(
                lower, steps, precision=lax.Precision.HIGHEST, preferred_element_type=F32
            )
            acrosses[b] = runs[b].T
        lows, mixes, sides, weighteds, reads, ends = [], [], [], [], [], []
        for b, h in pairs:
            q = unit(mixed(0, h, b))
            k = unit(mixed(1, h, b))
            v = mixed(2, h, b)
            beta = betas[b][:, h : h + 1]
            down = runs[b][:, heads + h : heads + h + 1]
            along = acrosses[b][heads + h : heads + h + 1, :]
            last = down[BLOCK - 1 : BLOCK, :]
            decay = jnp.where(within, jnp.exp(jnp.minimum(down - along, 0.0)), 0.0)
            grams = dot3(jnp.concatenate([q, k], axis=0), k, ((1,), (1,)))
            mixes.append(decay * grams[:BLOCK])
            lows.append(jnp.where(before, beta * decay * grams[BLOCK:], 0.0))
            growth = jnp.exp(down)
            sides.append(jnp.concatenate([beta * v, (beta * growth) * k], axis=1))
            weighteds.append((jnp.exp(last - down) * k).T)
            reads.append(growth * q)
            ends.append(jnp.exp(last))
        inverses = [eye - jnp.where((row // 2 == col // 2), low, 0.0) for low in lows]
        span = 2
        while span < BLOCK:
            linked = (row // (2 * span) == col // (2 * span)) & (row // span > col // span)
            shares = [split(inv) for inv in inverses]
            middles = [
                dot3(jnp.where(linked, low, 0.0), share) for low, share in zip(lows, shares)
            ]
            inverses = [
                inv - dot3(share, middle)
                for inv, share, middle in zip(inverses, shares, middles)
            ]
            span *= 2
        midway()
        solved = [split(dot3(inv, side)) for inv, side in zip(inverses, sides)]
        found = {}
        for i, (b, h) in enumerate(pairs):
            got = dot3(weighteds[i], solved[i])
            transit = ends[i] * eye - got[:, dim:]
            reader[h, b, pl.ds(BLOCK, dim), :] = transit.astype(BF16)
            maps[h, b] = got[:, :dim]
            found[b, h] = (transit, got[:, :dim])

        def outputs():
            for i, (b, h) in enumerate(pairs):
                got = dot3(mixes[i], solved[i])
                local[h, pl.ds(b * BLOCK, BLOCK), :] = got[:, :dim]
                reader[h, b, pl.ds(0, BLOCK), :] = (reads[i] - got[:, dim:]).astype(BF16)

        return found, outputs

    def columns_of(m):
        return pl.ds(pl.multiple_of((me ^ m) * columns, LANES), columns)

    own = pltpu.make_async_copy(w_ref.at[:, columns_of(0)], w_buf.at[0], own_sem)
    moves = {
        m: remote(
            w_ref.at[:, columns_of(m)], w_buf.at[m], w_send.at[m], w_recv.at[m], (seq, me ^ m)
        )
        for m in range(1, n)
    }
    far = sorted(range(2, n), key=lambda m: (-low_bit(m), m))
    joined = [None] * heads
    for g in range(GROUPS):
        mine = range(g * PER_GROUP, (g + 1) * PER_GROUP)
        for m in far:
            for c in mine:
                if (m, "in", c) not in hops:
                    arrive(m, c)
            add(m, g)
        if g == 0:
            add_prior()

        def midway():
            if g == 0:
                own.start()
                for m in far:
                    moves[m].start()
            if g + 1 < GROUPS:
                for m in far:
                    if low_bit(m) > 1:
                        c = (g + 1) * PER_GROUP
                        arrive(m, c)
                        hops[m, "in", c] = None

        found, outputs = block_terms(g, midway)
        for h in range(heads):
            for b in range(g * group_blocks, (g + 1) * group_blocks):
                transit, carried = found[b, h]
                if joined[h] is None:
                    joined[h] = jnp.concatenate([transit, carried], axis=1)
                else:
                    moved = dot3(transit, joined[h])
                    joined[h] = jnp.concatenate(
                        [moved[:, :dim], moved[:, dim:] + carried], axis=1
                    )
        if g + 1 < GROUPS:
            outputs()
        else:
            for h in range(heads):
                slab[h] = joined[h].astype(slab.dtype)

    swaps = [
        remote(slab.at[h], pair_buf.at[h], pair_sem.at[0, h], pair_sem.at[1, h], (mate, me))
        for h in range(heads)
    ]
    for swap in swaps:
        swap.start()
    moves[1].start()

    outputs()

    firsts, comps = [], []
    for h in range(heads):
        swaps[h].wait()
        here = slab[h].astype(F32)
        there = pair_buf[h].astype(F32)
        first = jnp.where(is_odd, there, here)
        second = jnp.where(is_odd, here, there)
        moved = dot(second[:, :dim], first)
        comps.append((moved[:, :dim], moved[:, dim:] + second[:, dim:]))
        firsts.append(first)
    sends = [
        remote(go_buf.at[h], in_buf.at[h], chain_send.at[h], chain_recv.at[h], (seq + 2, me))
        for h in range(heads)
    ]

    @pl.when(jnp.logical_not(far_before))
    def _():
        in_buf[...] = jnp.zeros(in_buf.shape, in_buf.dtype)

    for h in range(heads):

        @pl.when(far_before)
        def _():
            sends[h].wait_recv()

        @pl.when(far_next)
        def _():
            go_buf[h] = (dot(comps[h][0], in_buf[h]) + comps[h][1]).astype(go_buf.dtype)
            sends[h].start()

    states = []
    for h in range(heads):
        arrived = in_buf[h].astype(F32)
        later = dot(firsts[h][:, :dim], arrived) + firsts[h][:, dim:]
        states.append(jnp.where(is_odd, later, arrived))

    lifts = {}

    def lift(m, bit, b):
        got = m | bit
        return remote(
            hid.at[m, b], hid.at[got, b], h_send.at[got, b], h_recv.at[got, b], (seq, me ^ bit)
        )

    def forward(m, b):
        limit = n if m == 0 else low_bit(m)
        for bit in bits:
            if bit < limit:
                lifts[m | bit, b] = lift(m, bit, b)
                lifts[m | bit, b].start()

    for b in range(blocks):
        for h in range(heads):
            got = dot(reader[h, b], states[h])
            states[h] = got[BLOCK:] + maps[h, b]
            head_out = got[:BLOCK] + local[h, pl.ds(b * BLOCK, BLOCK), :]
            gate = raw[pl.ds(PRIOR + b * BLOCK, BLOCK), pl.ds(3 * width + h * dim, dim)]
            scaled = head_out * lax.rsqrt(
                jnp.mean(head_out * head_out, axis=-1, keepdims=True) + norm_floor
            )
            hid[0, b, :, pl.ds(h * dim, dim)] = (
                scaled * gain[...] * (gate * jax.nn.sigmoid(gate))
            ).astype(BF16)
        forward(0, b)

    own.wait()
    for move in moves.values():
        move.wait()
    order = sorted(range(1, n), key=lambda m: (m != 1, -low_bit(m), m))
    for b in range(blocks):
        total = jnp.dot(hid[0, b], w_buf[0], preferred_element_type=F32)
        for m in order:
            lifts[m, b].wait_recv()
            forward(m, b)
            total = total + jnp.dot(hid[m, b], w_buf[m], preferred_element_type=F32)
        out_ref[pl.ds(b * BLOCK, BLOCK), :] = total.astype(BF16)

    for key, copy in hops.items():
        if copy is not None:
            copy.wait_send()
    for copy in lifts.values():
        copy.wait_send()

    @pl.when(has_next)
    def _():
        for tail in tails:
            tail.wait_send()

    @pl.when(far_next)
    def _():
        for send in sends:
            send.wait_send()


def on_device(
    seqs, n,
    layer_in, query_weight, key_weight, value_weight, gate_weight, beta_weight, decay_weight,
    conv_weight, decay_log, beta_bias, decay_bias, norm_gain, out_weight,
):
    tokens, feats = layer_in.shape
    model, width = query_weight.shape
    heads = beta_weight.shape[1]
    dim = width // heads
    blocks = tokens // BLOCK
    total_width = 4 * width + LANES
    columns = out_weight.shape[1] // n
    vmem = pl.BlockSpec(memory_space=pltpu.VMEM)
    anywhere = pl.BlockSpec(memory_space=pl.ANY)
    dma = pltpu.SemaphoreType.DMA
    sends_each = GROUPS * PER_GROUP
    wire = BF16 if seqs <= 8 else F32
    return pl.pallas_call(
        functools.partial(layer_kernel, seqs, n, heads),
        out_shape=jax.ShapeDtypeStruct((tokens, columns), BF16),
        in_specs=[anywhere] * 13,
        out_specs=vmem,
        scratch_shapes=[
            pltpu.VMEM((model, total_width), BF16),
            pltpu.VMEM((LANES, model), F32),
            pltpu.VMEM((tokens, feats), BF16),
            pltpu.VMEM((n, tokens, feats), BF16),
            pltpu.VMEM((n, PRIOR, feats), BF16),
            pltpu.VMEM((PRIOR + tokens, total_width), F32),
            pltpu.VMEM((heads, tokens, dim), F32),
            pltpu.VMEM((heads, blocks, BLOCK + dim, dim), BF16),
            pltpu.VMEM((heads, blocks, dim, dim), F32),
            pltpu.VMEM((heads, dim, 2 * dim), wire),
            pltpu.VMEM((n, width, columns), BF16),
            pltpu.VMEM((heads, dim, 2 * dim), wire),
            pltpu.VMEM((heads, dim, dim), wire),
            pltpu.VMEM((heads, dim, dim), wire),
            pltpu.VMEM((n, blocks, BLOCK, width), BF16),
            pltpu.VMEM((heads, model), BF16),
            pltpu.VMEM((heads, model), BF16),
            pltpu.VMEM((conv_weight.shape[1], conv_weight.shape[0], width), F32),
            pltpu.VMEM((1, dim), F32),
            pltpu.SMEM((heads,), F32),
            pltpu.SMEM((heads,), F32),
            pltpu.SMEM((heads,), F32),
            dma((4,)),
            dma((7,)),
            dma(()),
            dma((n, sends_each)),
            dma((n, sends_each)),
            dma((n,)),
            dma((n,)),
            dma(()),
            dma((n,)),
            dma((n,)),
            dma((2, heads)),
            dma((heads,)),
            dma((heads,)),
            dma((n, blocks)),
            dma((n, blocks)),
        ],
        compiler_params=pltpu.CompilerParams(
            collective_id=0, has_side_effects=True, vmem_limit_bytes=60 * 1024 * 1024
        ),
    )(
        layer_in, query_weight, key_weight, value_weight, gate_weight,
        beta_weight.T, decay_weight.T, conv_weight.transpose(1, 0, 2),
        decay_log, beta_bias, decay_bias, norm_gain[None], out_weight,
    )


def solution(mesh):
    return jax.shard_map(
        functools.partial(on_device, mesh.shape["seq"], mesh.shape["head"]),
        mesh=mesh,
        in_specs=(
            P("seq", "head"),
            P(None, "head"),
            P(None, "head"),
            P(None, "head"),
            P(None, "head"),
            P(None, "head"),
            P(None, "head"),
            P(None, None, "head"),
            P("head"),
            P("head"),
            P("head"),
            P(),
            P("head", None),
        ),
        out_specs=P("seq", "head"),
        check_vma=False,
    )
```

```python
import functools

import jax
import jax.numpy as jnp
from jax import lax
from jax.experimental import pallas as pl
from jax.experimental.pallas import tpu as pltpu
from jax.sharding import PartitionSpec as P

BLOCK = 128
PRIOR = 16
LANES = 128
GROUPS = 2
PER_GROUP = 2
MESH = pl.DeviceIdType.MESH
F32 = jnp.float32
BF16 = jnp.bfloat16
norm_floor = 0.0001


def bits_below(limit):
    found = []
    bit = limit // 2
    while bit:
        found.append(bit)
        bit //= 2
    return found


def low_bit(value):
    return value & -value


def meet(peers):
    barrier = pltpu.get_barrier_semaphore()
    expected = 0
    for present, device in peers:
        if present is True:
            pl.semaphore_signal(barrier, inc=1, device_id=device, device_id_type=MESH)
            expected = expected + 1
        else:

            @pl.when(present)
            def _():
                pl.semaphore_signal(barrier, inc=1, device_id=device, device_id_type=MESH)

            expected = expected + present.astype(jnp.int32)
    pl.semaphore_wait(barrier, expected)


def remote(source, target, send_sem, recv_sem, device):
    return pltpu.make_async_remote_copy(
        src_ref=source,
        dst_ref=target,
        send_sem=send_sem,
        recv_sem=recv_sem,
        device_id=device,
        device_id_type=MESH,
    )


def dot(left, right, contract=((1,), (0,))):
    return lax.dot_general(
        left.astype(BF16), right.astype(BF16), (contract, ((), ())), preferred_element_type=F32
    )


def split(value):
    high = value.astype(BF16)
    return high, (value - high.astype(F32)).astype(BF16)


def dot3(left, right, contract=((1,), (0,))):
    lh, ll = left if isinstance(left, tuple) else split(left)
    rh, rl = right if isinstance(right, tuple) else split(right)
    axis = contract[1][0]
    both = dot(jnp.concatenate([lh, lh], axis=1), jnp.concatenate([rh, rl], axis=axis), contract)
    return both + dot(ll, rh, contract)


def layer_kernel(
    seqs, n, heads,
    x_ref, wq, wk, wv, wg, beta_in, step_in, taps_in, rates_in, bias_in, shift_in, gain_in, w_ref,
    out_ref,
    w_all, w_flat, x_own, buf, prior, raw, local, reader, maps, slab,
    w_buf, pair_buf, go_buf, in_buf, hid,
    beta_ref, step_ref, taps, gain, rates, beta_bias, decay_bias,
    load_sem, small_sem, x_sem, x_send, x_recv, p_send, p_recv, own_sem, w_send, w_recv,
    pair_sem, chain_send, chain_recv, h_send, h_recv,
):
    seq = lax.axis_index("seq")
    me = lax.axis_index("head")
    tokens, feats = x_ref.shape
    width = wq.shape[1]
    dim = LANES
    blocks = tokens // BLOCK
    columns = out_ref.shape[1]
    sends_each = GROUPS * PER_GROUP
    rows = tokens // sends_each
    group_rows = tokens // GROUPS
    group_blocks = blocks // GROUPS
    bits = bits_below(n)

    loads = [pltpu.make_async_copy(x_ref, x_own, x_sem)]
    for i, w in enumerate((wq, wk, wv, wg)):
        loads.append(
            pltpu.make_async_copy(w, w_all.at[:, pl.ds(i * width, width)], load_sem.at[i])
        )
    smalls = [
        pltpu.make_async_copy(source, target, small_sem.at[i])
        for i, (source, target) in enumerate((
            (beta_in, beta_ref), (step_in, step_ref), (taps_in, taps), (gain_in, gain),
            (rates_in, rates), (bias_in, beta_bias), (shift_in, decay_bias),
        ))
    ]
    for load in loads + smalls:
        load.start()
    has_next = seq < seqs - 1
    has_before = seq > 0
    far_next = seq < seqs - 2
    far_before = seq >= 2
    odd = seq % 2
    is_odd = odd == 1
    mate = seq + 1 - 2 * odd
    peers = [(True, (seq, me ^ m)) for m in range(1, n)]
    peers += [(has_next, (seq + 1, me ^ m)) for m in range(n)]
    peers += [(has_before, (seq - 1, me ^ m)) for m in range(n)]
    peers += [(far_next, (seq + 2, me)), (far_before, (seq - 2, me))]
    meet(peers)

    def hop(m, bit, c):
        piece = pl.ds(c * rows, rows)
        source = x_ref.at[piece] if m == 0 else buf.at[m, piece]
        got = m | bit
        return remote(
            source, buf.at[got, piece], x_send.at[got, c], x_recv.at[got, c], (seq, me ^ bit)
        )

    tails = [
        remote(
            x_ref.at[pl.ds(tokens - PRIOR, PRIOR)],
            prior.at[m],
            p_send.at[m],
            p_recv.at[m],
            (seq + 1, me ^ m),
        )
        for m in range(n)
    ]

    @pl.when(has_next)
    def _():
        for tail in tails:
            tail.start()

    hops = {}
    for bit in bits:
        for c in range(sends_each):
            hops[bit, c] = hop(0, bit, c)
            hops[bit, c].start()
    for load in smalls:
        load.wait()
    w_flat[...] = jnp.zeros(w_flat.shape, F32)
    w_flat[pl.ds(0, heads), :] = beta_ref[...].astype(F32)
    w_flat[pl.ds(heads, heads), :] = step_ref[...].astype(F32)
    for i in range(w_flat.shape[1] // LANES):
        piece = pl.ds(i * LANES, LANES)
        w_all[piece, pl.ds(4 * width, LANES)] = w_flat[:, piece].T.astype(BF16)
    for load in loads:
        load.wait()

    def weights_of(m):
        start = pl.multiple_of((me ^ m) * feats, LANES)
        return w_all[pl.ds(start, feats), :]

    def arrive(m, c):
        hops[m, c].wait_recv()
        for bit in bits:
            if bit < low_bit(m):
                hops[m | bit, c] = hop(m, bit, c)
                hops[m | bit, c].start()

    def add(m, g):
        piece = pl.ds(g * group_rows, group_rows)
        here = pl.ds(PRIOR + g * group_rows, group_rows)
        values = x_own[piece, :] if m == 0 else buf[m, piece, :]
        term = jnp.dot(values, weights_of(m), preferred_element_type=F32)
        if m == 0:
            raw[here, :] = term
        else:
            raw[here, :] = raw[here, :] + term

    for g in range(GROUPS):
        add(0, g)
    for g in range(GROUPS):
        for c in range(g * PER_GROUP, (g + 1) * PER_GROUP):
            arrive(1, c)
        add(1, g)

    def add_prior():
        @pl.when(has_before)
        def _():
            total = jnp.zeros((PRIOR, raw.shape[1]), F32)
            for m in range(n):
                tails[m].wait_recv()
                total = total + jnp.dot(prior[m], weights_of(m), preferred_element_type=F32)
            raw[pl.ds(0, PRIOR), :] = total

        @pl.when(jnp.logical_not(has_before))
        def _():
            raw[pl.ds(0, PRIOR), :] = jnp.zeros((PRIOR, raw.shape[1]), F32)

    row = lax.broadcasted_iota(jnp.int32, (BLOCK, BLOCK), 0)
    col = lax.broadcasted_iota(jnp.int32, (BLOCK, BLOCK), 1)
    within = row >= col
    before = row > col
    eye = (row == col).astype(F32)
    lower = within.astype(F32)
    lane = lax.broadcasted_iota(jnp.int32, (1, LANES), 1)
    offset = jnp.zeros((1, LANES), F32)
    rate = jnp.zeros((1, LANES), F32)
    for h in range(heads):
        offset = jnp.where(lane == h, beta_bias[h], offset)
        offset = jnp.where(lane == heads + h, decay_bias[h], offset)
        rate = jnp.where(lane == heads + h, rates[h], rate)
    rate = -jnp.exp(rate)

    def mixed(kind, h, b):
        base = kind * width + h * dim
        start = PRIOR + b * BLOCK
        total = None
        for s in range(taps.shape[1]):
            tap = taps[kind, pl.ds(s, 1), pl.ds(h * dim, dim)]
            term = tap * raw[pl.ds(start - s, BLOCK), pl.ds(base, dim)]
            total = term if total is None else total + term
        return total * jax.nn.sigmoid(total)

    def unit(values):
        return values * lax.rsqrt(jnp.sum(values * values, axis=-1, keepdims=True) + 1.0)

    def block_terms(g, midway):
        pairs = [(b, h) for b in range(g * group_blocks, (g + 1) * group_blocks)
                 for h in range(heads)]
        betas, runs, acrosses = {}, {}, {}
        for b in range(g * group_blocks, (g + 1) * group_blocks):
            small = raw[pl.ds(PRIOR + b * BLOCK, BLOCK), pl.ds(4 * width, LANES)] + offset
            betas[b] = jax.nn.sigmoid(small)
            steps = rate * (jnp.maximum(small, 0.0) + jnp.log1p(jnp.exp(-jnp.abs(small))))
            runs[b] = jnp.dot(
                lower, steps, precision=lax.Precision.HIGHEST, preferred_element_type=F32
            )
            acrosses[b] = runs[b].T
        lows, mixes, sides, weighteds, reads, ends = [], [], [], [], [], []
        for b, h in pairs:
            q = unit(mixed(0, h, b))
            k = unit(mixed(1, h, b))
            v = mixed(2, h, b)
            beta = betas[b][:, h : h + 1]
            down = runs[b][:, heads + h : heads + h + 1]
            along = acrosses[b][heads + h : heads + h + 1, :]
            last = down[BLOCK - 1 : BLOCK, :]
            decay = jnp.where(within, jnp.exp(jnp.minimum(down - along, 0.0)), 0.0)
            grams = dot3(jnp.concatenate([q, k], axis=0), k, ((1,), (1,)))
            mixes.append(decay * grams[:BLOCK])
            lows.append(jnp.where(before, beta * decay * grams[BLOCK:], 0.0))
            growth = jnp.exp(down)
            sides.append(jnp.concatenate([beta * v, (beta * growth) * k], axis=1))
            weighteds.append((jnp.exp(last - down) * k).T)
            reads.append(growth * q)
            ends.append(jnp.exp(last))
        inverses = [eye - jnp.where((row // 2 == col // 2), low, 0.0) for low in lows]
        span = 2
        while span < BLOCK:
            linked = (row // (2 * span) == col // (2 * span)) & (row // span > col // span)
            shares = [split(inv) for inv in inverses]
            middles = [
                dot3(jnp.where(linked, low, 0.0), share) for low, share in zip(lows, shares)
            ]
            inverses = [
                inv - dot3(share, middle)
                for inv, share, middle in zip(inverses, shares, middles)
            ]
            span *= 2
        midway()
        solved = [split(dot3(inv, side)) for inv, side in zip(inverses, sides)]
        found = {}
        for i, (b, h) in enumerate(pairs):
            got = dot3(weighteds[i], solved[i])
            transit = ends[i] * eye - got[:, dim:]
            reader[h, b, pl.ds(BLOCK, dim), :] = transit.astype(BF16)
            maps[h, b] = got[:, :dim]
            found[b, h] = (transit, got[:, :dim])

        def outputs():
            for i, (b, h) in enumerate(pairs):
                got = dot3(mixes[i], solved[i])
                local[h, pl.ds(b * BLOCK, BLOCK), :] = got[:, :dim]
                reader[h, b, pl.ds(0, BLOCK), :] = (reads[i] - got[:, dim:]).astype(BF16)

        return found, outputs

    def columns_of(m):
        return pl.ds(pl.multiple_of((me ^ m) * columns, LANES), columns)

    own = pltpu.make_async_copy(w_ref.at[:, columns_of(0)], w_buf.at[0], own_sem)
    moves = {
        m: remote(
            w_ref.at[:, columns_of(m)], w_buf.at[m], w_send.at[m], w_recv.at[m], (seq, me ^ m)
        )
        for m in range(1, n)
    }
    far = sorted(range(2, n), key=lambda m: (-low_bit(m), m))
    joined = [None] * heads
    for g in range(GROUPS):
        mine = range(g * PER_GROUP, (g + 1) * PER_GROUP)
        for m in far:
            for c in mine:
                if (m, "in", c) not in hops:
                    arrive(m, c)
            add(m, g)
        if g == 0:
            add_prior()

        def midway():
            if g == 0:
                own.start()
                for m in far:
                    moves[m].start()
            if g + 1 < GROUPS:
                for m in far:
                    if low_bit(m) > 1:
                        c = (g + 1) * PER_GROUP
                        arrive(m, c)
                        hops[m, "in", c] = None

        found, outputs = block_terms(g, midway)
        for h in range(heads):
            for b in range(g * group_blocks, (g + 1) * group_blocks):
                transit, carried = found[b, h]
                if joined[h] is None:
                    joined[h] = jnp.concatenate([transit, carried], axis=1)
                else:
                    moved = dot3(transit, joined[h])
                    joined[h] = jnp.concatenate(
                        [moved[:, :dim], moved[:, dim:] + carried], axis=1
                    )
        if g + 1 < GROUPS:
            outputs()
        else:
            for h in range(heads):
                slab[h] = joined[h].astype(slab.dtype)

    swaps = [
        remote(slab.at[h], pair_buf.at[h], pair_sem.at[0, h], pair_sem.at[1, h], (mate, me))
        for h in range(heads)
    ]
    for swap in swaps:
        swap.start()
    moves[1].start()

    outputs()
    for h in range(heads):
        place = pl.ds(PRIOR, tokens), pl.ds(3 * width + h * dim, dim)
        gate = raw[place]
        raw[place] = gain[...] * (gate * jax.nn.sigmoid(gate))

    firsts, comps = [], []
    for h in range(heads):
        swaps[h].wait()
        here = slab[h].astype(F32)
        there = pair_buf[h].astype(F32)
        first = jnp.where(is_odd, there, here)
        second = jnp.where(is_odd, here, there)
        moved = dot(second[:, :dim], first)
        comps.append((moved[:, :dim], moved[:, dim:] + second[:, dim:]))
        firsts.append(first)
    sends = [
        remote(go_buf.at[h], in_buf.at[h], chain_send.at[h], chain_recv.at[h], (seq + 2, me))
        for h in range(heads)
    ]

    @pl.when(jnp.logical_not(far_before))
    def _():
        in_buf[...] = jnp.zeros(in_buf.shape, in_buf.dtype)

    for h in range(heads):

        @pl.when(far_before)
        def _():
            sends[h].wait_recv()

        @pl.when(far_next)
        def _():
            go_buf[h] = (dot(comps[h][0], in_buf[h]) + comps[h][1]).astype(go_buf.dtype)
            sends[h].start()

    states = []
    for h in range(heads):
        arrived = in_buf[h].astype(F32)
        later = dot(firsts[h][:, :dim], arrived) + firsts[h][:, dim:]
        states.append(jnp.where(is_odd, later, arrived))

    lifts = {}

    def lift(m, bit, b):
        got = m | bit
        return remote(
            hid.at[m, b], hid.at[got, b], h_send.at[got, b], h_recv.at[got, b], (seq, me ^ bit)
        )

    def forward(m, b):
        limit = n if m == 0 else low_bit(m)
        for bit in bits:
            if bit < limit:
                lifts[m | bit, b] = lift(m, bit, b)
                lifts[m | bit, b].start()

    for b in range(blocks):
        for h in range(heads):
            got = dot(reader[h, b], states[h])
            states[h] = got[BLOCK:] + maps[h, b]
            head_out = got[:BLOCK] + local[h, pl.ds(b * BLOCK, BLOCK), :]
            gate = raw[pl.ds(PRIOR + b * BLOCK, BLOCK), pl.ds(3 * width + h * dim, dim)]
            scaled = head_out * lax.rsqrt(
                jnp.mean(head_out * head_out, axis=-1, keepdims=True) + norm_floor
            )
            hid[0, b, :, pl.ds(h * dim, dim)] = (
                scaled * gate
            ).astype(BF16)
        forward(0, b)

    own.wait()
    for move in moves.values():
        move.wait()
    order = sorted(range(1, n), key=lambda m: (m != 1, -low_bit(m), m))
    for b in range(blocks):
        total = jnp.dot(hid[0, b], w_buf[0], preferred_element_type=F32)
        for m in order:
            lifts[m, b].wait_recv()
            forward(m, b)
            total = total + jnp.dot(hid[m, b], w_buf[m], preferred_element_type=F32)
        out_ref[pl.ds(b * BLOCK, BLOCK), :] = total.astype(BF16)

    for key, copy in hops.items():
        if copy is not None:
            copy.wait_send()
    for copy in lifts.values():
        copy.wait_send()

    @pl.when(has_next)
    def _():
        for tail in tails:
            tail.wait_send()

    @pl.when(far_next)
    def _():
        for send in sends:
            send.wait_send()


def on_device(
    seqs, n,
    layer_in, query_weight, key_weight, value_weight, gate_weight, beta_weight, decay_weight,
    conv_weight, decay_log, beta_bias, decay_bias, norm_gain, out_weight,
):
    tokens, feats = layer_in.shape
    model, width = query_weight.shape
    heads = beta_weight.shape[1]
    dim = width // heads
    blocks = tokens // BLOCK
    total_width = 4 * width + LANES
    columns = out_weight.shape[1] // n
    vmem = pl.BlockSpec(memory_space=pltpu.VMEM)
    anywhere = pl.BlockSpec(memory_space=pl.ANY)
    dma = pltpu.SemaphoreType.DMA
    sends_each = GROUPS * PER_GROUP
    wire = BF16 if seqs <= 8 else F32
    return pl.pallas_call(
        functools.partial(layer_kernel, seqs, n, heads),
        out_shape=pltpu.VMEM((tokens, columns), BF16),
        in_specs=[anywhere] * 13,
        out_specs=vmem,
        scratch_shapes=[
            pltpu.VMEM((model, total_width), BF16),
            pltpu.VMEM((LANES, model), F32),
            pltpu.VMEM((tokens, feats), BF16),
            pltpu.VMEM((n, tokens, feats), BF16),
            pltpu.VMEM((n, PRIOR, feats), BF16),
            pltpu.VMEM((PRIOR + tokens, total_width), F32),
            pltpu.VMEM((heads, tokens, dim), F32),
            pltpu.VMEM((heads, blocks, BLOCK + dim, dim), BF16),
            pltpu.VMEM((heads, blocks, dim, dim), F32),
            pltpu.VMEM((heads, dim, 2 * dim), wire),
            pltpu.VMEM((n, width, columns), BF16),
            pltpu.VMEM((heads, dim, 2 * dim), wire),
            pltpu.VMEM((heads, dim, dim), wire),
            pltpu.VMEM((heads, dim, dim), wire),
            pltpu.VMEM((n, blocks, BLOCK, width), BF16),
            pltpu.VMEM((heads, model), BF16),
            pltpu.VMEM((heads, model), BF16),
            pltpu.VMEM((conv_weight.shape[1], conv_weight.shape[0], width), F32),
            pltpu.VMEM((1, dim), F32),
            pltpu.SMEM((heads,), F32),
            pltpu.SMEM((heads,), F32),
            pltpu.SMEM((heads,), F32),
            dma((4,)),
            dma((7,)),
            dma(()),
            dma((n, sends_each)),
            dma((n, sends_each)),
            dma((n,)),
            dma((n,)),
            dma(()),
            dma((n,)),
            dma((n,)),
            dma((2, heads)),
            dma((heads,)),
            dma((heads,)),
            dma((n, blocks)),
            dma((n, blocks)),
        ],
        compiler_params=pltpu.CompilerParams(
            collective_id=0, has_side_effects=True, vmem_limit_bytes=60 * 1024 * 1024
        ),
    )(
        layer_in, query_weight, key_weight, value_weight, gate_weight,
        beta_weight.T, decay_weight.T, conv_weight.transpose(1, 0, 2),
        decay_log, beta_bias, decay_bias, norm_gain[None], out_weight,
    )


def solution(mesh):
    return jax.shard_map(
        functools.partial(on_device, mesh.shape["seq"], mesh.shape["head"]),
        mesh=mesh,
        in_specs=(
            P("seq", "head"),
            P(None, "head"),
            P(None, "head"),
            P(None, "head"),
            P(None, "head"),
            P(None, "head"),
            P(None, "head"),
            P(None, None, "head"),
            P("head"),
            P("head"),
            P("head"),
            P(),
            P("head", None),
        ),
        out_specs=P("seq", "head"),
        check_vma=False,
    )
```
